16 devices in a mesh: rep: 2 (over y, z), dp: 8 (over x, core).
Axes of the slice: x: 4, y: 2, z: 1, core: 2. Of those that a mesh axis runs over, the one named last changes fastest.
The devices are a block of a 4x4x8 slice.
Arguments:
- a: bfloat16 [16, 4, 2048, 1024], P(('rep', 'dp')), parts along dimension 0
- g: bfloat16 [16, 4, 2048, 3200], P(('rep', 'dp')), parts along dimension 0
Outputs:
- output: bfloat16 [8, 1024, 3200], P('rep'), parts along dimension 0
There are 2 independent parts. The reference program is written for one: setup_inputs(seed, part) draws one part's arguments, and reference() takes and returns one part's arrays. A program takes and returns all parts, laid end to end along the dimension named above; each array names one.
All inputs are finite; a program needn't handle non-finite values.
Results may differ from the reference program's by a relative error of at most 0.012.
Values are sent between devices in bfloat16 or wider.
A program may use at most 768 MiB of HBM per device.

```python
import jax
import jax.numpy as jnp
from jax import lax

DEVICES = 8
MATRICES = 4
TOKENS = 2048
D = 1024
FF = 3200


def setup_inputs(seed: int = 0, part: int = 0) -> dict:
    ka, kg, ks = (jax.random.fold_in(k, part) for k in jax.random.split(jax.random.key(seed), 3))
    size = 2.0 ** jax.random.uniform(ks, (DEVICES, MATRICES, 1, 1), jnp.float32, -1.0, 1.0)
    a = jax.random.normal(ka, (DEVICES, MATRICES, TOKENS, D), jnp.float32)
    g = size * jax.random.normal(kg, (DEVICES, MATRICES, TOKENS, FF), jnp.float32) * (DEVICES * TOKENS) ** -0.5
    return {"a": a.astype(jnp.bfloat16), "g": g.astype(jnp.bfloat16)}


def reference(a, g):
    def take(so_far, one):
        return so_far + jnp.einsum("ntd,ntf->ndf", *one, preferred_element_type=jnp.float32), None

    return lax.scan(take, jnp.zeros((MATRICES, D, FF), jnp.float32), (a, g))[0].astype(jnp.bfloat16)
```

```python
import functools

import jax
import jax.numpy as jnp
from jax import lax
from jax.experimental import pallas as pl
from jax.experimental.pallas import tpu as pltpu
from jax.sharding import PartitionSpec as P

MESH = pl.DeviceIdType.MESH
CORES = 2
LEFT, RIGHT, MATE = 0, 1, 2
SLOTS = 8
F32, BF16 = jnp.float32, jnp.bfloat16


def kernel(
    chips, wide, a_hbm, g_hbm, out,
    a_buf, g_buf, mine, give, take, keep, ab_out, ab_in, c_out, c_in,
    a_sem, g_sem, give_sem, take_sem, ab_sent, ab_got, c_sent, c_got,
    own_sent, own_got, far_sent, far_got, fwd_sent, fwd_got,
):
    matrices, rows, columns = out.shape
    blocks = columns // wide
    units = matrices * blocks
    half = rows // CORES
    own = half // chips
    sub = own // 2

    me = lax.axis_index("dp")
    x, core = me // CORES, me % CORES
    xl, xr, opp = (x + chips - 1) % chips, (x + 1) % chips, (x + 2) % chips
    dev = {LEFT: xl * CORES + core, RIGHT: xr * CORES + core, MATE: x * CORES + 1 - core}
    base, mate_base = core * half, (1 - core) * half

    def load_a(n):
        return pltpu.make_async_copy(a_hbm.at[0, n], a_buf.at[n % 2], a_sem.at[n % 2])

    def load_g(u):
        return pltpu.make_async_copy(
            g_hbm.at[0, u // blocks, :, pl.ds(pl.multiple_of(u % blocks * wide, 128), wide)],
            g_buf.at[u % 2],
            g_sem.at[u % 2],
        )

    def remote(src, dst, sent, got, to):
        return pltpu.make_async_remote_copy(
            src_ref=src, dst_ref=dst, send_sem=sent, recv_sem=got,
            device_id={"dp": dev[to]}, device_id_type=MESH,
        )

    def place(u, row, count):
        return out.at[
            u // blocks,
            pl.ds(pl.multiple_of(row, sub), count),
            pl.ds(pl.multiple_of(u % blocks * wide, 128), wide),
        ]

    def hand(u):
        s = u % 4
        return remote(give.at[u % 2], take.at[s], give_sem.at[s], take_sem.at[s], MATE)

    def ab(u, to):
        s = u % SLOTS
        return remote(ab_out.at[u % 4, to], ab_in.at[s, to], ab_sent.at[s, to], ab_got.at[s, to], to)

    def c(u, to):
        s = u % SLOTS
        return remote(c_out.at[u % 4, to], c_in.at[s, to], c_sent.at[s, to], c_got.at[s, to], to)

    def owned(u, to):
        s, ref = u % SLOTS, place(u, base + x * own, own)
        return remote(ref, ref, own_sent.at[s, to], own_got.at[s, to], to)

    def far(u, to):
        s = u % SLOTS
        row = base + (xl * own if to == RIGHT else xr * own + sub)
        ref = place(u, row, sub)
        return remote(ref, ref, far_sent.at[s, to], far_got.at[s, to], to)

    def forward(u, k):
        s = u % SLOTS
        ref = place(u, base + (xl, xr, opp)[k] * own, own)
        return remote(ref, ref, fwd_sent.at[s, k], fwd_got.at[s, k], MATE)

    load_a(0).start()
    load_g(0).start()
    barrier = pltpu.get_barrier_semaphore()
    for to in (LEFT, RIGHT, MATE):
        pl.semaphore_signal(barrier, inc=1, device_id={"dp": dev[to]}, device_id_type=MESH)
    pl.semaphore_wait(barrier, 3)

    def multiply(u, row, count):
        return lax.dot_general(
            a_buf[u // blocks % 2, :, pl.ds(pl.multiple_of(row, 128), count)],
            g_buf[u % 2],
            (((0,), (0,)), ((), ())),
            preferred_element_type=F32,
        )

    def iteration(t, carry):
        def stage(lag):
            u = t - lag
            return u, pl.when((u >= 0) & (u < units))

        u_next, on_next = stage(-1)

        @on_next
        def _():
            load_g(u_next).start()

        @pl.when((t % blocks == 0) & (t // blocks + 1 < matrices))
        def _():
            load_a(t // blocks + 1).start()

        u_b, on_b = stage(1)

        @on_b
        def _():
            u, s, k = u_b, u_b % 4, u_b % 2
            hand(u).wait()

            @pl.when(u >= 4)
            def _():
                for to in (LEFT, RIGHT):
                    ab(u - 4, to).wait_send()

            def total(owner, offset):
                where = pl.ds(pl.multiple_of(owner * own + offset, sub), sub)
                return mine[k, where, :] + take[s, where, :].astype(F32)

            ab_out[s, LEFT, :sub, :] = total(opp, 0).astype(BF16)
            ab_out[s, LEFT, sub:, :] = total(xl, sub).astype(BF16)
            ab(u, LEFT).start()
            ab_out[s, RIGHT, :sub, :] = total(opp, sub).astype(BF16)
            ab_out[s, RIGHT, sub:, :] = total(xr, 0).astype(BF16)
            ab(u, RIGHT).start()
            keep[s, 0] = total(xl, 0)
            keep[s, 1] = total(xr, sub)
            keep[s, 2] = total(x, 0)
            keep[s, 3] = total(x, sub)

        u_c, on_c = stage(2)

        @on_c
        def _():
            u, s, r = u_c, u_c % 4, u_c % SLOTS

            @pl.when(u >= 4)
            def _():
                for to in (LEFT, RIGHT):
                    c(u - 4, to).wait_send()

            for to in (LEFT, RIGHT):
                ab(u, to).wait_recv()
                c_out[s, to] = (keep[s, to] + ab_in[r, to, :sub, :].astype(F32)).astype(BF16)
                c(u, to).start()

        u_d, on_d = stage(3)

        @on_d
        def _():
            u, s, r = u_d, u_d % 4, u_d % SLOTS
            cols = pl.ds(pl.multiple_of(u % blocks * wide, 128), wide)
            for k in (0, 1):
                c(u, k).wait_recv()
                total = keep[s, 2 + k] + c_in[r, k].astype(F32) + ab_in[r, 1 - k, sub:, :].astype(F32)
                row = pl.ds(pl.multiple_of(base + x * own + k * sub, sub), sub)
                out[u // blocks, row, cols] = total.astype(BF16)
            for to in (LEFT, RIGHT, MATE):
                owned(u, to).start()

        u_e, on_e = stage(4)

        @on_e
        def _():
            owned(u_e, RIGHT).wait_recv()
            far(u_e, RIGHT).start()
            owned(u_e, LEFT).wait_recv()
            far(u_e, LEFT).start()
            forward(u_e, 0).start()
            forward(u_e, 1).start()

        u_g, on_g = stage(5)

        @on_g
        def _():
            far(u_g, RIGHT).wait_recv()
            far(u_g, LEFT).wait_recv()
            forward(u_g, 2).start()

        u_h, on_h = stage(6)

        @on_h
        def _():
            for to in (LEFT, RIGHT, MATE):
                owned(u_h, to).wait_send()
            owned(u_h, MATE).wait_recv()
            for to in (LEFT, RIGHT):
                far(u_h, to).wait_send()
            for k in range(3):
                forward(u_h, k).wait()

        u_a, on_a = stage(0)

        @on_a
        def _():
            u = u_a

            @pl.when(u % blocks == 0)
            def _():
                load_a(u // blocks).wait()

            load_g(u).wait()

            @pl.loop(0, half, step=256)
            def _(i):
                give[u % 2, pl.ds(pl.multiple_of(i, 256), 256), :] = multiply(u, mate_base + i, 256).astype(BF16)

            hand(u).start()

            @pl.loop(0, half, step=256)
            def _(i):
                mine[u % 2, pl.ds(pl.multiple_of(i, 256), 256), :] = multiply(u, base + i, 256)

        return carry

    lax.fori_loop(0, units + 7, iteration, 0)
    for i in range(4):
        for to in (LEFT, RIGHT):
            ab(units - 4 + i, to).wait_send()
            c(units - 4 + i, to).wait_send()


def solution(mesh):
    chips = mesh.shape["dp"] // CORES

    def device(a, g):
        _, matrices, tokens, rows = a.shape
        columns = g.shape[-1]
        wide = 128 * next(k for k in (5, 6, 4, 3, 2, 1) if columns % (128 * k) == 0)
        half = rows // CORES
        own = half // chips
        sub = own // 2
        dma = pltpu.SemaphoreType.DMA
        sums = pl.pallas_call(
            functools.partial(kernel, chips, wide),
            out_shape=pltpu.VMEM((matrices, rows, columns), BF16),
            in_specs=[pl.BlockSpec(memory_space=pltpu.HBM)] * 2,
            out_specs=pl.BlockSpec(memory_space=pltpu.VMEM),
            scratch_shapes=[
                pltpu.VMEM((2, tokens, rows), BF16),
                pltpu.VMEM((2, tokens, wide), BF16),
                pltpu.VMEM((2, half, wide), F32),
                pltpu.VMEM((2, half, wide), BF16),
                pltpu.VMEM((4, half, wide), BF16),
                pltpu.VMEM((4, 4, sub, wide), F32),
                pltpu.VMEM((4, 2, own, wide), BF16),
                pltpu.VMEM((SLOTS, 2, own, wide), BF16),
                pltpu.VMEM((4, 2, sub, wide), BF16),
                pltpu.VMEM((SLOTS, 2, sub, wide), BF16),
                dma((2,)), dma((2,)), dma((4,)), dma((4,)),
                dma((SLOTS, 2)), dma((SLOTS, 2)), dma((SLOTS, 2)), dma((SLOTS, 2)),
                dma((SLOTS, 3)), dma((SLOTS, 3)), dma((SLOTS, 2)), dma((SLOTS, 2)),
                dma((SLOTS, 3)), dma((SLOTS, 3)),
            ],
            compiler_params=pltpu.CompilerParams(
                collective_id=0, has_side_effects=True, vmem_limit_bytes=37 * 2**20
            ),
            cost_estimate=pl.CostEstimate(
                flops=2 * matrices * tokens * rows * columns,
                bytes_accessed=2 * matrices * tokens * (rows + columns),
                transcendentals=0,
            ),
        )(a, g)

        def store(held, result, sem):
            copies = [pltpu.make_async_copy(held.at[n], result.at[n], sem.at[n]) for n in range(matrices)]
            for copy in copies:
                copy.start()
            for copy in copies:
                copy.wait()

        return pl.pallas_call(
            store,
            out_shape=jax.ShapeDtypeStruct(sums.shape, BF16),
            in_specs=[pl.BlockSpec(memory_space=pltpu.VMEM)],
            out_specs=pl.BlockSpec(memory_space=pltpu.HBM),
            scratch_shapes=[dma((matrices,))],
            compiler_params=pltpu.CompilerParams(vmem_limit_bytes=2**20),
        )(pltpu.with_memory_space_constraint(sums, pltpu.VMEM))

    return jax.shard_map(
        device, mesh=mesh, in_specs=(P(("rep", "dp")), P(("rep", "dp"))), out_specs=P("rep"), check_vma=False
    )
```

```python
import functools

import jax
import jax.numpy as jnp
from jax import lax
from jax.experimental import pallas as pl
from jax.experimental.pallas import tpu as pltpu
from jax.sharding import PartitionSpec as P

MESH = pl.DeviceIdType.MESH
CORES = 2
LEFT, RIGHT, MATE = 0, 1, 2
SLOTS = 5
TILE = 512
LAG = 2
F32, BF16 = jnp.float32, jnp.bfloat16


def cut(columns):
    blocks = max(columns // TILE, 1)
    return blocks, blocks // 2, columns - (blocks - 1) * TILE


def kernel(
    chips, a_hbm, g_hbm, out,
    a_buf, g_buf, mine, give, take, keep, ab_out, ab_in, c_out, c_in,
    a_sem, g_sem, give_sem, take_sem, ab_sent, ab_got, c_sent, c_got,
    own_got, far_got, out_sent, mate_sent, mate_got,
):
    matrices, rows, columns = out.shape
    blocks, middle, wide = cut(columns)
    units = matrices * blocks
    half = rows // CORES
    own = half // chips
    sub = own // 2

    me = lax.axis_index("dp")
    x, core = me // CORES, me % CORES
    xl, xr, opp = (x + chips - 1) % chips, (x + 1) % chips, (x + 2) % chips
    dev = {LEFT: xl * CORES + core, RIGHT: xr * CORES + core, MATE: x * CORES + 1 - core}
    base, mate_base = core * half, (1 - core) * half

    def columns_of(u, w):
        j = u % blocks
        return pl.ds(pl.multiple_of(j * TILE + (j + blocks - 1 - middle) // blocks * (wide - TILE), 128), w)

    def load_a(n, h):
        where = pl.ds(pl.multiple_of((mate_base, base)[h], 128), half)
        return pltpu.make_async_copy(a_hbm.at[0, n, :, where], a_buf.at[n % 2, h], a_sem.at[h])

    def load_g(u, w):
        return pltpu.make_async_copy(
            g_hbm.at[0, u // blocks, :, columns_of(u, w)], g_buf.at[u % 2, :, pl.ds(0, w)], g_sem.at[u % 2]
        )

    def remote(src, dst, sent, got, to):
        return pltpu.make_async_remote_copy(
            src_ref=src, dst_ref=dst, send_sem=sent, recv_sem=got,
            device_id={"dp": dev[to]}, device_id_type=MESH,
        )

    def place(u, w, row, count):
        return out.at[u // blocks, pl.ds(pl.multiple_of(row, sub), count), columns_of(u, w)]

    def hand(u, w):
        s, cols = u % 2, pl.ds(0, w)
        return remote(give.at[s, :, cols], take.at[s, :, cols], give_sem.at[s], take_sem.at[s], MATE)

    def ab(u, w, to):
        s, k, cols = u % SLOTS, u % 2, pl.ds(0, w)
        return remote(ab_out.at[k, to, :, cols], ab_in.at[s, to, :, cols], ab_sent.at[k], ab_got.at[s, to], to)

    def c(u, w, to):
        s, k, cols = u % SLOTS, u % 2, pl.ds(0, w)
        return remote(c_out.at[k, to, :, cols], c_in.at[s, to, :, cols], c_sent.at[k], c_got.at[s], to)

    def owned(u, w, to):
        s, ref = u % SLOTS, place(u, w, base + x * own, own)
        if to == MATE:
            return remote(ref, ref, mate_sent, mate_got, to)
        return remote(ref, ref, out_sent, own_got.at[s, to], to)

    def far(u, w, to):
        row = base + (xl * own if to == RIGHT else xr * own + sub)
        ref = place(u, w, row, sub)
        return remote(ref, ref, out_sent, far_got.at[u % SLOTS], to)

    def forward(u, w, k):
        ref = place(u, w, base + (xl, xr, opp)[k] * own, own)
        return remote(ref, ref, mate_sent, mate_got, MATE)

    def wait_for(ref, sem):
        pltpu.make_async_copy(ref, ref, sem).wait()

    def run(stage, u, also=True):
        here = (u >= 0) & (u < units) & also
        if wide == TILE:
            pl.when(here)(lambda: stage(u, TILE))
        else:
            pl.when(here & (u % blocks != middle))(lambda: stage(u, TILE))
            pl.when(here & (u % blocks == middle))(lambda: stage(u, wide))

    def multiply(u, w, h):
        return lax.dot_general(
            a_buf[u // blocks % 2, h],
            g_buf[u % 2, :, :w],
            (((0,), (0,)), ((), ())),
            preferred_element_type=F32,
        )

    def stage_a(u, w):
        load_g(u, w).wait()
        give[u % 2, :, :w] = multiply(u, w, 0).astype(BF16)

    def stage_a2(u, w):
        hand(u, w).start()
        mine[:, :w] = multiply(u, w, 1)

    def stage_b(u, w):
        k = u % 2
        hand(u, w).wait()

        def total(owner, offset):
            where = pl.ds(pl.multiple_of(owner * own + offset, sub), sub)
            return mine[where, :w] + take[k, where, :w].astype(F32)

        ab_out[k, LEFT, :sub, :w] = total(opp, 0).astype(BF16)
        ab_out[k, LEFT, sub:, :w] = total(xl, sub).astype(BF16)
        ab(u, w, LEFT).start()
        ab_out[k, RIGHT, :sub, :w] = total(opp, sub).astype(BF16)
        ab_out[k, RIGHT, sub:, :w] = total(xr, 0).astype(BF16)
        ab(u, w, RIGHT).start()
        s = u % SLOTS
        keep[s, 0, :, :w] = total(xl, 0)
        keep[s, 1, :, :w] = total(xr, sub)
        keep[s, 2, :, :w] = total(x, 0)
        keep[s, 3, :, :w] = total(x, sub)

    def stage_b0(u, w):
        wait_for(ab_out.at[u % 2, :, :, pl.ds(0, w)], ab_sent.at[u % 2])

    def stage_c(u, w):
        s, k = u % SLOTS, u % 2
        for to in (LEFT, RIGHT):
            ab(u, w, to).wait_recv()
            c_out[k, to, :, :w] = (keep[s, to, :, :w] + ab_in[s, to, :sub, :w].astype(F32)).astype(BF16)
            c(u, w, to).start()
        for to in (LEFT, RIGHT):
            keep[s, 3 - to, :, :w] += ab_in[s, to, sub:, :w].astype(F32)

    def stage_c0(u, w):
        wait_for(c_out.at[u % 2, :, :, pl.ds(0, w)], c_sent.at[u % 2])

    def stage_d(u, w):
        s = u % SLOTS
        wait_for(c_in.at[s, :, :, pl.ds(0, w)], c_got.at[s])
        for k in (0, 1):
            total = keep[s, 2 + k, :, :w] + c_in[s, k, :, :w].astype(F32)
            row = pl.ds(pl.multiple_of(base + x * own + k * sub, sub), sub)
            out[u // blocks, row, columns_of(u, w)] = total.astype(BF16)
        for to in (LEFT, RIGHT, MATE):
            owned(u, w, to).start()

    def stage_e(u, w):
        owned(u, w, RIGHT).wait_recv()
        far(u, w, RIGHT).start()
        owned(u, w, LEFT).wait_recv()
        far(u, w, LEFT).start()
        forward(u, w, 0).start()
        forward(u, w, 1).start()

    def stage_g(u, w):
        wait_for(place(u, w, base + opp * own, own), far_got.at[u % SLOTS])
        forward(u, w, 2).start()

    barrier = pltpu.get_barrier_semaphore()
    load_a(0, 0).start()
    load_g(0, TILE).start()
    load_a(0, 1).start()
    for to in (LEFT, RIGHT, MATE):
        pl.semaphore_signal(barrier, inc=1, device_id={"dp": dev[to]}, device_id_type=MESH)

    def iteration(t, carry):
        n, first = t // blocks, (t % blocks == 0) & (t < units)
        run(lambda u, w: load_g(u, w).start(), t + 1)

        @pl.when((t % blocks == 1) & (n + 1 < matrices))
        def _():
            for h in (0, 1):
                load_a(n + 1, h).start()

        pl.when(first)(lambda: load_a(n, 0).wait())
        run(stage_a, t)
        pl.when(t == 0)(lambda: pl.semaphore_wait(barrier, 3))
        pl.when(first)(lambda: load_a(n, 1).wait())
        run(stage_a2, t)
        run(stage_b0, t - 2)
        run(stage_b, t)
        run(stage_c0, t - 2 - LAG)
        run(stage_c, t - LAG)
        run(stage_d, t - LAG - 1)
        run(stage_e, t - LAG - 2)
        run(stage_g, t - LAG - 3)
        return carry

    lax.fori_loop(0, units + LAG + 3, iteration, 0)
    wait_for(out.at[:, pl.ds(pl.multiple_of(base, half), half), :], mate_sent)
    wait_for(out.at[:, pl.ds(0, 3 * own), :], out_sent)
    wait_for(out.at[:, pl.ds(pl.multiple_of(mate_base, half), half), :], mate_got)


def solution(mesh):
    chips = mesh.shape["dp"] // CORES

    def device(a, g):
        _, matrices, tokens, rows = a.shape
        columns = g.shape[-1]
        wide = cut(columns)[2]
        half = rows // CORES
        own = half // chips
        sub = own // 2
        dma = pltpu.SemaphoreType.DMA
        sums = pl.pallas_call(
            functools.partial(kernel, chips),
            out_shape=pltpu.VMEM((matrices, rows, columns), BF16),
            in_specs=[pl.BlockSpec(memory_space=pltpu.HBM)] * 2,
            out_specs=pl.BlockSpec(memory_space=pltpu.VMEM),
            scratch_shapes=[
                pltpu.VMEM((2, CORES, tokens, half), BF16),
                pltpu.VMEM((2, tokens, wide), BF16),
                pltpu.VMEM((half, wide), F32),
                pltpu.VMEM((2, half, wide), BF16),
                pltpu.VMEM((2, half, wide), BF16),
                pltpu.VMEM((SLOTS, 4, sub, wide), F32),
                pltpu.VMEM((2, 2, own, wide), BF16),
                pltpu.VMEM((SLOTS, 2, own, wide), BF16),
                pltpu.VMEM((2, 2, sub, wide), BF16),
                pltpu.VMEM((SLOTS, 2, sub, wide), BF16),
                dma((2,)), dma((2,)), dma((2,)), dma((2,)), dma((2,)), dma((SLOTS, 2)), dma((2,)), dma((SLOTS,)),
                dma((SLOTS, 2)), dma((SLOTS,)), dma, dma, dma,
            ],
            compiler_params=pltpu.CompilerParams(
                collective_id=0, has_side_effects=True, vmem_limit_bytes=37 * 2**20
            ),
            cost_estimate=pl.CostEstimate(
                flops=2 * matrices * tokens * rows * columns,
                bytes_accessed=2 * matrices * tokens * (rows + columns),
                transcendentals=0,
            ),
        )(a, g)

        def store(held, result, sem):
            copies = [pltpu.make_async_copy(held.at[n], result.at[n], sem.at[n]) for n in range(matrices)]
            for copy in copies:
                copy.start()
            for copy in copies:
                copy.wait()

        return pl.pallas_call(
            store,
            out_shape=jax.ShapeDtypeStruct(sums.shape, BF16),
            in_specs=[pl.BlockSpec(memory_space=pltpu.VMEM)],
            out_specs=pl.BlockSpec(memory_space=pltpu.HBM),
            scratch_shapes=[dma((matrices,))],
            compiler_params=pltpu.CompilerParams(vmem_limit_bytes=2**20),
        )(pltpu.with_memory_space_constraint(sums, pltpu.VMEM))

    return jax.shard_map(
        device, mesh=mesh, in_specs=(P(("rep", "dp")), P(("rep", "dp"))), out_specs=P("rep"), check_vma=False
    )
```

```python
import functools

import jax
import jax.numpy as jnp
from jax import lax
from jax.experimental import pallas as pl
from jax.experimental.pallas import tpu as pltpu
from jax.sharding import PartitionSpec as P

MESH = pl.DeviceIdType.MESH
CORES = 2
LEFT, RIGHT, MATE = 0, 1, 2
SLOTS = 5
TILE = 512
F32, BF16 = jnp.float32, jnp.bfloat16


def cut(columns):
    blocks = max(columns // TILE, 1)
    return blocks, blocks // 2, columns - (blocks - 1) * TILE


def kernel(
    chips, a_hbm, g_hbm, out,
    a_buf, g_buf, mine, give, take, keep, ab_out, ab_in, c_out, c_in,
    a_sem, g_sem, give_sem, take_sem, ab_sent, ab_got, c_sent, c_got,
    own_got, far_got, out_sent, mate_sent, mate_got,
):
    matrices, rows, columns = out.shape
    tokens = a_hbm.shape[2]
    blocks, middle, wide = cut(columns)
    units = matrices * blocks
    half = rows // CORES
    own = half // chips
    sub = own // 2

    me = lax.axis_index("dp")
    x, core = me // CORES, me % CORES
    xl, xr, opp = (x + chips - 1) % chips, (x + 1) % chips, (x + 2) % chips
    dev = {LEFT: xl * CORES + core, RIGHT: xr * CORES + core, MATE: x * CORES + 1 - core}
    base, mate_base = core * half, (1 - core) * half

    def columns_of(u, w):
        j = u % blocks
        return pl.ds(pl.multiple_of(j * TILE + (j + blocks - 1 - middle) // blocks * (wide - TILE), 128), w)

    def load_a(n, h):
        where = pl.ds(pl.multiple_of((mate_base, base)[h], 128), half)
        return pltpu.make_async_copy(a_hbm.at[0, n, :, where], a_buf.at[n % 2, h], a_sem.at[h])

    def load_g(u, w):
        return pltpu.make_async_copy(
            g_hbm.at[0, u // blocks, :, columns_of(u, w)], g_buf.at[u % 2, :, pl.ds(0, w)], g_sem.at[u % 2]
        )

    def load_first(k):
        part = pl.ds(k * (tokens // 2), tokens // 2)
        where = pl.ds(pl.multiple_of(mate_base, 128), half)
        return (
            pltpu.make_async_copy(a_hbm.at[0, 0, part, where], a_buf.at[0, 0, part], a_sem.at[2 * k]),
            pltpu.make_async_copy(
                g_hbm.at[0, 0, part, pl.ds(0, TILE)], g_buf.at[0, part, pl.ds(0, TILE)], g_sem.at[2 * k]
            ),
        )

    def remote(src, dst, sent, got, to):
        return pltpu.make_async_remote_copy(
            src_ref=src, dst_ref=dst, send_sem=sent, recv_sem=got,
            device_id={"dp": dev[to]}, device_id_type=MESH,
        )

    def place(u, w, row, count):
        return out.at[u // blocks, pl.ds(pl.multiple_of(row, sub), count), columns_of(u, w)]

    def hand(u, w):
        s, cols = u % 2, pl.ds(0, w)
        return remote(give.at[s, :, cols], take.at[s, :, cols], give_sem.at[s], take_sem.at[s], MATE)

    def ab(u, w, to):
        s, k, cols = u % SLOTS, u % 2, pl.ds(0, w)
        return remote(ab_out.at[k, to, :, cols], ab_in.at[s, to, :, cols], ab_sent.at[k], ab_got.at[s, to], to)

    def c(u, w, to):
        s, k, cols = u % SLOTS, u % 2, pl.ds(0, w)
        return remote(c_out.at[k, to, :, cols], c_in.at[s, to, :, cols], c_sent.at[k], c_got.at[s], to)

    def owned(u, w, to):
        s, ref = u % SLOTS, place(u, w, base + x * own, own)
        if to == MATE:
            return remote(ref, ref, mate_sent, mate_got, to)
        return remote(ref, ref, out_sent, own_got.at[s, to], to)

    def far(u, w, to):
        row = base + (xl * own if to == RIGHT else xr * own + sub)
        ref = place(u, w, row, sub)
        return remote(ref, ref, out_sent, far_got.at[u % SLOTS], to)

    def forward(u, w, k):
        ref = place(u, w, base + (xl, xr, opp)[k] * own, own)
        return remote(ref, ref, mate_sent, mate_got, MATE)

    def wait_for(ref, sem):
        pltpu.make_async_copy(ref, ref, sem).wait()

    def run(stage, u, also=True):
        here = (u >= 0) & (u < units) & also
        if wide == TILE:
            pl.when(here)(lambda: stage(u, TILE))
        else:
            pl.when(here & (u % blocks != middle))(lambda: stage(u, TILE))
            pl.when(here & (u % blocks == middle))(lambda: stage(u, wide))

    def run_late(stage, u):
        run(stage, u, u < units - 1)
        run(stage, units - 1, u == units - 2)

    def multiply(u, w, h, start=0, end=tokens):
        return lax.dot_general(
            a_buf[u // blocks % 2, h, start:end],
            g_buf[u % 2, start:end, :w],
            (((0,), (0,)), ((), ())),
            preferred_element_type=F32,
        )

    def stage_a(u, w):
        load_g(u, w).wait()
        give[u % 2, :, :w] = multiply(u, w, 0).astype(BF16)

    def stage_a2(u, w):
        hand(u, w).start()
        mine[:, :w] = multiply(u, w, 1)

    def stage_b(u, w):
        k = u % 2
        hand(u, w).wait()

        def total(owner, offset):
            where = pl.ds(pl.multiple_of(owner * own + offset, sub), sub)
            return mine[where, :w] + take[k, where, :w].astype(F32)

        ab_out[k, LEFT, :sub, :w] = total(opp, 0).astype(BF16)
        ab_out[k, LEFT, sub:, :w] = total(xl, sub).astype(BF16)
        ab(u, w, LEFT).start()
        ab_out[k, RIGHT, :sub, :w] = total(opp, sub).astype(BF16)
        ab_out[k, RIGHT, sub:, :w] = total(xr, 0).astype(BF16)
        ab(u, w, RIGHT).start()
        s = u % SLOTS
        keep[s, 0, :, :w] = total(xl, 0)
        keep[s, 1, :, :w] = total(xr, sub)
        keep[s, 2, :, :w] = total(x, 0)
        keep[s, 3, :, :w] = total(x, sub)

    def stage_b0(u, w):
        wait_for(ab_out.at[u % 2, :, :, pl.ds(0, w)], ab_sent.at[u % 2])

    def stage_c(u, w):
        s, k = u % SLOTS, u % 2
        for to in (LEFT, RIGHT):
            ab(u, w, to).wait_recv()
            c_out[k, to, :, :w] = (keep[s, to, :, :w] + ab_in[s, to, :sub, :w].astype(F32)).astype(BF16)
            c(u, w, to).start()
        for to in (LEFT, RIGHT):
            keep[s, 3 - to, :, :w] += ab_in[s, to, sub:, :w].astype(F32)

    def stage_c0(u, w):
        wait_for(c_out.at[u % 2, :, :, pl.ds(0, w)], c_sent.at[u % 2])

    def stage_d(u, w):
        s = u % SLOTS
        wait_for(c_in.at[s, :, :, pl.ds(0, w)], c_got.at[s])
        for k in (0, 1):
            total = keep[s, 2 + k, :, :w] + c_in[s, k, :, :w].astype(F32)
            row = pl.ds(pl.multiple_of(base + x * own + k * sub, sub), sub)
            out[u // blocks, row, columns_of(u, w)] = total.astype(BF16)
        for to in (LEFT, RIGHT, MATE):
            owned(u, w, to).start()

    def stage_e(u, w):
        owned(u, w, RIGHT).wait_recv()
        far(u, w, RIGHT).start()
        owned(u, w, LEFT).wait_recv()
        far(u, w, LEFT).start()
        forward(u, w, 0).start()
        forward(u, w, 1).start()

    def stage_g(u, w):
        wait_for(place(u, w, base + opp * own, own), far_got.at[u % SLOTS])
        forward(u, w, 2).start()

    barrier = pltpu.get_barrier_semaphore()
    for k in (0, 1):
        for copy in load_first(k):
            copy.start()
    load_a(0, 1).start()
    for to in (LEFT, RIGHT, MATE):
        pl.semaphore_signal(barrier, inc=1, device_id={"dp": dev[to]}, device_id_type=MESH)
    for copy in load_first(0):
        copy.wait()
    mine[:, :TILE] = multiply(0, TILE, 0, 0, tokens // 2)
    for copy in load_first(1):
        copy.wait()
    give[0, :, :TILE] = (mine[:, :TILE] + multiply(0, TILE, 0, tokens // 2)).astype(BF16)
    pl.semaphore_wait(barrier, 3)

    def iteration(t, carry):
        n, first = t // blocks, (t % blocks == 0) & (t < units)
        run(lambda u, w: load_g(u, w).start(), t + 1)

        @pl.when((t % blocks == 1) & (n + 1 < matrices))
        def _():
            for h in (0, 1):
                load_a(n + 1, h).start()

        pl.when(first & (t > 0))(lambda: load_a(n, 0).wait())
        run(stage_a, t, t > 0)
        pl.when(first)(lambda: load_a(n, 1).wait())
        run(stage_a2, t)
        run(stage_c0, t - 4, t - 4 != units - 3)
        run(stage_c0, units - 3, t == units)
        run_late(stage_c, t - 2)
        run(stage_b0, t - 2)
        run(stage_b, t)
        run_late(stage_d, t - 3)
        run_late(stage_e, t - 4)
        run_late(stage_g, t - 5)
        return carry

    lax.fori_loop(0, units + 4, iteration, 0)
    wait_for(out.at[:, pl.ds(pl.multiple_of(base, half), half), :], mate_sent)
    wait_for(out.at[:, pl.ds(0, 3 * own), :], out_sent)
    wait_for(out.at[:, pl.ds(pl.multiple_of(mate_base, half), half), :], mate_got)


def solution(mesh):
    chips = mesh.shape["dp"] // CORES

    def device(a, g):
        _, matrices, tokens, rows = a.shape
        columns = g.shape[-1]
        wide = cut(columns)[2]
        half = rows // CORES
        own = half // chips
        sub = own // 2
        dma = pltpu.SemaphoreType.DMA
        sums = pl.pallas_call(
            functools.partial(kernel, chips),
            out_shape=pltpu.VMEM((matrices, rows, columns), BF16),
            in_specs=[pl.BlockSpec(memory_space=pltpu.HBM)] * 2,
            out_specs=pl.BlockSpec(memory_space=pltpu.VMEM),
            scratch_shapes=[
                pltpu.VMEM((2, CORES, tokens, half), BF16),
                pltpu.VMEM((2, tokens, wide), BF16),
                pltpu.VMEM((half, wide), F32),
                pltpu.VMEM((2, half, wide), BF16),
                pltpu.VMEM((2, half, wide), BF16),
                pltpu.VMEM((SLOTS, 4, sub, wide), F32),
                pltpu.VMEM((2, 2, own, wide), BF16),
                pltpu.VMEM((SLOTS, 2, own, wide), BF16),
                pltpu.VMEM((2, 2, sub, wide), BF16),
                pltpu.VMEM((SLOTS, 2, sub, wide), BF16),
                dma((3,)), dma((3,)), dma((2,)), dma((2,)), dma((2,)), dma((SLOTS, 2)), dma((2,)), dma((SLOTS,)),
                dma((SLOTS, 2)), dma((SLOTS,)), dma, dma, dma,
            ],
            compiler_params=pltpu.CompilerParams(
                collective_id=0, has_side_effects=True, vmem_limit_bytes=37 * 2**20
            ),
            cost_estimate=pl.CostEstimate(
                flops=2 * matrices * tokens * rows * columns,
                bytes_accessed=2 * matrices * tokens * (rows + columns),
                transcendentals=0,
            ),
        )(a, g)

        def store(held, result, sem):
            copies = [pltpu.make_async_copy(held.at[n], result.at[n], sem.at[n]) for n in range(matrices)]
            for copy in copies:
                copy.start()
            for copy in copies:
                copy.wait()

        return pl.pallas_call(
            store,
            out_shape=jax.ShapeDtypeStruct(sums.shape, BF16),
            in_specs=[pl.BlockSpec(memory_space=pltpu.VMEM)],
            out_specs=pl.BlockSpec(memory_space=pltpu.HBM),
            scratch_shapes=[dma((matrices,))],
            compiler_params=pltpu.CompilerParams(vmem_limit_bytes=2**20),
        )(pltpu.with_memory_space_constraint(sums, pltpu.VMEM))

    return jax.shard_map(
        device, mesh=mesh, in_specs=(P(("rep", "dp")), P(("rep", "dp"))), out_specs=P("rep"), check_vma=False
    )
```

```python
import functools

import jax
import jax.numpy as jnp
from jax import lax
from jax.experimental import pallas as pl
from jax.experimental.pallas import tpu as pltpu
from jax.sharding import PartitionSpec as P

MESH = pl.DeviceIdType.MESH
CORES = 2
LEFT, RIGHT, MATE = 0, 1, 2
SLOTS = 5
TILE = 512
F32, BF16 = jnp.float32, jnp.bfloat16


def cut(columns):
    blocks = max(columns // TILE, 1)
    return blocks, 2 * blocks // 3, columns - (blocks - 1) * TILE


def kernel(
    chips, a_hbm, g_hbm, out,
    a_buf, g_buf, mine, give, take, keep, ab_out, ab_in, c_out, c_in,
    a_sem, g_sem, give_sem, take_sem, ab_sent, ab_got, c_sent, c_got,
    own_got, far_got, out_sent, mate_sent, mate_got,
):
    matrices, rows, columns = out.shape
    tokens = a_hbm.shape[2]
    blocks, fat, wide = cut(columns)
    units = matrices * blocks
    half = rows // CORES
    own = half // chips
    sub = own // 2

    me = lax.axis_index("dp")
    x, core = me // CORES, me % CORES
    xl, xr, opp = (x + chips - 1) % chips, (x + 1) % chips, (x + 2) % chips
    dev = {LEFT: xl * CORES + core, RIGHT: xr * CORES + core, MATE: x * CORES + 1 - core}
    base, mate_base = core * half, (1 - core) * half

    def columns_of(u, w):
        j = u % blocks
        return pl.ds(pl.multiple_of(j * TILE + (j + blocks - 1 - fat) // blocks * (wide - TILE), 128), w)

    def load_a(n, h):
        where = pl.ds(pl.multiple_of((mate_base, base)[h], 128), half)
        return pltpu.make_async_copy(a_hbm.at[0, n, :, where], a_buf.at[n % 2, h], a_sem.at[h])

    def load_g(u, w):
        return pltpu.make_async_copy(
            g_hbm.at[0, u // blocks, :, columns_of(u, w)], g_buf.at[u % 2, :, pl.ds(0, w)], g_sem.at[u % 2]
        )

    def load_first(k):
        part = pl.ds(k * (tokens // 2), tokens // 2)
        where = pl.ds(pl.multiple_of(mate_base, 128), half)
        return (
            pltpu.make_async_copy(a_hbm.at[0, 0, part, where], a_buf.at[0, 0, part], a_sem.at[2 * k]),
            pltpu.make_async_copy(
                g_hbm.at[0, 0, part, pl.ds(0, TILE)], g_buf.at[0, part, pl.ds(0, TILE)], g_sem.at[2 * k]
            ),
        )

    def remote(src, dst, sent, got, to):
        return pltpu.make_async_remote_copy(
            src_ref=src, dst_ref=dst, send_sem=sent, recv_sem=got,
            device_id={"dp": dev[to]}, device_id_type=MESH,
        )

    def place(u, w, row, count):
        return out.at[u // blocks, pl.ds(pl.multiple_of(row, sub), count), columns_of(u, w)]

    def hand(u, w):
        s, cols = u % 2, pl.ds(0, w)
        return remote(give.at[s, :, cols], take.at[s, :, cols], give_sem.at[s], take_sem.at[s], MATE)

    def ab(u, w, to):
        s, k, cols = u % SLOTS, u % 2, pl.ds(0, w)
        return remote(ab_out.at[k, to, :, cols], ab_in.at[s, to, :, cols], ab_sent.at[k], ab_got.at[s, to], to)

    def c(u, w, to):
        s, k, cols = u % SLOTS, u % 2, pl.ds(0, w)
        return remote(c_out.at[k, to, :, cols], c_in.at[s, to, :, cols], c_sent.at[k], c_got.at[s], to)

    def owned(u, w, to):
        s, ref = u % SLOTS, place(u, w, base + x * own, own)
        if to == MATE:
            return remote(ref, ref, mate_sent, mate_got, to)
        return remote(ref, ref, out_sent, own_got.at[s, to], to)

    def far(u, w, to):
        row = base + (xl * own if to == RIGHT else xr * own + sub)
        ref = place(u, w, row, sub)
        return remote(ref, ref, out_sent, far_got.at[u % SLOTS], to)

    def forward(u, w, k):
        ref = place(u, w, base + (xl, xr, opp)[k] * own, own)
        return remote(ref, ref, mate_sent, mate_got, MATE)

    def wait_for(ref, sem):
        pltpu.make_async_copy(ref, ref, sem).wait()

    def run(stage, u, also=True):
        here = (u >= 0) & (u < units) & also
        if wide == TILE:
            pl.when(here)(lambda: stage(u, TILE))
        else:
            pl.when(here & (u % blocks != fat))(lambda: stage(u, TILE))
            pl.when(here & (u % blocks == fat))(lambda: stage(u, wide))

    def run_late(stage, u):
        run(stage, u, u < units - 1)
        run(stage, units - 1, u == units - 2)

    def multiply(u, w, h, start=0, end=tokens):
        return lax.dot_general(
            a_buf[u // blocks % 2, h, start:end],
            g_buf[u % 2, start:end, :w],
            (((0,), (0,)), ((), ())),
            preferred_element_type=F32,
        )

    def stage_a(u, w):
        load_g(u, w).wait()
        give[u % 2, :, :w] = multiply(u, w, 0).astype(BF16)

    def stage_a2(u, w):
        hand(u, w).start()
        mine[:, :w] = multiply(u, w, 1)

    def stage_b(u, w):
        k = u % 2
        hand(u, w).wait()

        def total(owner, offset):
            where = pl.ds(pl.multiple_of(owner * own + offset, sub), sub)
            return mine[where, :w] + take[k, where, :w].astype(F32)

        ab_out[k, LEFT, :sub, :w] = total(opp, 0).astype(BF16)
        ab_out[k, LEFT, sub:, :w] = total(xl, sub).astype(BF16)
        ab(u, w, LEFT).start()
        ab_out[k, RIGHT, :sub, :w] = total(opp, sub).astype(BF16)
        ab_out[k, RIGHT, sub:, :w] = total(xr, 0).astype(BF16)
        ab(u, w, RIGHT).start()
        s = u % SLOTS
        keep[s, 0, :, :w] = total(xl, 0)
        keep[s, 1, :, :w] = total(xr, sub)
        keep[s, 2, :, :w] = total(x, 0)
        keep[s, 3, :, :w] = total(x, sub)

    def stage_b0(u, w):
        wait_for(ab_out.at[u % 2, :, :, pl.ds(0, w)], ab_sent.at[u % 2])

    def stage_c(u, w):
        s, k = u % SLOTS, u % 2
        for to in (LEFT, RIGHT):
            ab(u, w, to).wait_recv()
            c_out[k, to, :, :w] = (keep[s, to, :, :w] + ab_in[s, to, :sub, :w].astype(F32)).astype(BF16)
            c(u, w, to).start()
        for to in (LEFT, RIGHT):
            keep[s, 3 - to, :, :w] += ab_in[s, to, sub:, :w].astype(F32)

    def stage_c0(u, w):
        wait_for(c_out.at[u % 2, :, :, pl.ds(0, w)], c_sent.at[u % 2])

    def stage_d(u, w):
        s = u % SLOTS
        wait_for(c_in.at[s, :, :, pl.ds(0, w)], c_got.at[s])
        for k in (0, 1):
            total = keep[s, 2 + k, :, :w] + c_in[s, k, :, :w].astype(F32)
            row = pl.ds(pl.multiple_of(base + x * own + k * sub, sub), sub)
            out[u // blocks, row, columns_of(u, w)] = total.astype(BF16)
        for to in (LEFT, RIGHT, MATE):
            owned(u, w, to).start()

    def stage_e(u, w):
        owned(u, w, RIGHT).wait_recv()
        far(u, w, RIGHT).start()
        owned(u, w, LEFT).wait_recv()
        far(u, w, LEFT).start()
        forward(u, w, 0).start()
        forward(u, w, 1).start()

    def stage_g(u, w):
        wait_for(place(u, w, base + opp * own, own), far_got.at[u % SLOTS])
        forward(u, w, 2).start()

    barrier = pltpu.get_barrier_semaphore()
    for k in (0, 1):
        for copy in load_first(k):
            copy.start()
    load_a(0, 1).start()
    for to in (LEFT, RIGHT, MATE):
        pl.semaphore_signal(barrier, inc=1, device_id={"dp": dev[to]}, device_id_type=MESH)
    for copy in load_first(0):
        copy.wait()
    mine[:, :TILE] = multiply(0, TILE, 0, 0, tokens // 2)
    for copy in load_first(1):
        copy.wait()
    give[0, :, :TILE] = (mine[:, :TILE] + multiply(0, TILE, 0, tokens // 2)).astype(BF16)
    pl.semaphore_wait(barrier, 3)

    def iteration(t, carry):
        n, first = t // blocks, (t % blocks == 0) & (t < units)
        run(lambda u, w: load_g(u, w).start(), t + 1)

        @pl.when((t % blocks == 1) & (n + 1 < matrices))
        def _():
            for h in (0, 1):
                load_a(n + 1, h).start()

        pl.when(first & (t > 0))(lambda: load_a(n, 0).wait())
        run(stage_a, t, t > 0)
        pl.when(first)(lambda: load_a(n, 1).wait())
        run(stage_a2, t)
        run(stage_c0, t - 4, t - 4 != units - 3)
        run(stage_c0, units - 3, t == units)
        run_late(stage_c, t - 2)
        run(stage_b0, t - 2)
        run(stage_b, t)
        run_late(stage_d, t - 3)
        run_late(stage_e, t - 4)
        run_late(stage_g, t - 5)
        return carry

    lax.fori_loop(0, units + 4, iteration, 0)
    wait_for(out.at[:, pl.ds(pl.multiple_of(base, half), half), :], mate_sent)
    wait_for(out.at[:, pl.ds(0, 3 * own), :], out_sent)
    wait_for(out.at[:, pl.ds(pl.multiple_of(mate_base, half), half), :], mate_got)


def solution(mesh):
    chips = mesh.shape["dp"] // CORES

    def device(a, g):
        _, matrices, tokens, rows = a.shape
        columns = g.shape[-1]
        wide = cut(columns)[2]
        half = rows // CORES
        own = half // chips
        sub = own // 2
        dma = pltpu.SemaphoreType.DMA
        sums = pl.pallas_call(
            functools.partial(kernel, chips),
            out_shape=pltpu.VMEM((matrices, rows, columns), BF16),
            in_specs=[pl.BlockSpec(memory_space=pltpu.HBM)] * 2,
            out_specs=pl.BlockSpec(memory_space=pltpu.VMEM),
            scratch_shapes=[
                pltpu.VMEM((2, CORES, tokens, half), BF16),
                pltpu.VMEM((2, tokens, wide), BF16),
                pltpu.VMEM((half, wide), F32),
                pltpu.VMEM((2, half, wide), BF16),
                pltpu.VMEM((2, half, wide), BF16),
                pltpu.VMEM((SLOTS, 4, sub, wide), F32),
                pltpu.VMEM((2, 2, own, wide), BF16),
                pltpu.VMEM((SLOTS, 2, own, wide), BF16),
                pltpu.VMEM((2, 2, sub, wide), BF16),
                pltpu.VMEM((SLOTS, 2, sub, wide), BF16),
                dma((3,)), dma((3,)), dma((2,)), dma((2,)), dma((2,)), dma((SLOTS, 2)), dma((2,)), dma((SLOTS,)),
                dma((SLOTS, 2)), dma((SLOTS,)), dma, dma, dma,
            ],
            compiler_params=pltpu.CompilerParams(
                collective_id=0, has_side_effects=True, vmem_limit_bytes=37 * 2**20
            ),
            cost_estimate=pl.CostEstimate(
                flops=2 * matrices * tokens * rows * columns,
                bytes_accessed=2 * matrices * tokens * (rows + columns),
                transcendentals=0,
            ),
        )(a, g)

        def store(held, result, sem):
            parts = [(n, pl.ds(k * half // 2, half // 2)) for n in range(matrices) for k in range(2 * rows // half)]
            copies = [pltpu.make_async_copy(held.at[p], result.at[p], sem.at[i]) for i, p in enumerate(parts)]
            for copy in copies:
                copy.start()
            for copy in copies:
                copy.wait()

        return pl.pallas_call(
            store,
            out_shape=jax.ShapeDtypeStruct(sums.shape, BF16),
            in_specs=[pl.BlockSpec(memory_space=pltpu.VMEM)],
            out_specs=pl.BlockSpec(memory_space=pltpu.HBM),
            scratch_shapes=[dma((matrices * 2 * rows // half,))],
            compiler_params=pltpu.CompilerParams(vmem_limit_bytes=2**20),
        )(pltpu.with_memory_space_constraint(sums, pltpu.VMEM))

    return jax.shard_map(
        device, mesh=mesh, in_specs=(P(("rep", "dp")), P(("rep", "dp"))), out_specs=P("rep"), check_vma=False
    )
```

```python
import functools

import jax
import jax.numpy as jnp
from jax import lax
from jax.experimental import pallas as pl
from jax.experimental.pallas import tpu as pltpu
from jax.sharding import PartitionSpec as P

MESH = pl.DeviceIdType.MESH
CORES = 2
LEFT, RIGHT, MATE = 0, 1, 2
SLOTS = 5
TILE = 512
F32, BF16 = jnp.float32, jnp.bfloat16


def cut(columns):
    blocks = max(columns // TILE, 1)
    return blocks, 2 * blocks // 3, columns - (blocks - 1) * TILE


def kernel(
    chips, a_hbm, g_hbm, out,
    a_buf, g_buf, mine, give, take, keep, ab_out, ab_in, c_out, c_in,
    a_sem, g_sem, give_sem, take_sem, ab_sent, ab_got, c_sent, c_got,
    own_got, far_got, out_sent, mate_sent, mate_got,
):
    matrices, rows, columns = out.shape
    tokens = a_hbm.shape[2]
    blocks, fat, wide = cut(columns)
    units = matrices * blocks
    half = rows // CORES
    own = half // chips
    sub = own // 2

    me = lax.axis_index("dp")
    x, core = me // CORES, me % CORES
    xl, xr, opp = (x + chips - 1) % chips, (x + 1) % chips, (x + 2) % chips
    dev = {LEFT: xl * CORES + core, RIGHT: xr * CORES + core, MATE: x * CORES + 1 - core}
    base, mate_base = core * half, (1 - core) * half

    def columns_of(u, w):
        j = u % blocks
        return pl.ds(pl.multiple_of(j * TILE + (j + blocks - 1 - fat) // blocks * (wide - TILE), 128), w)

    def load_a(n, h):
        where = pl.ds(pl.multiple_of((mate_base, base)[h], 128), half)
        return pltpu.make_async_copy(a_hbm.at[0, n, :, where], a_buf.at[n % 2, h], a_sem.at[h])

    def load_g(u, w):
        return pltpu.make_async_copy(
            g_hbm.at[0, u // blocks, :, columns_of(u, w)], g_buf.at[u % 2, :, pl.ds(0, w)], g_sem.at[u % 2]
        )

    def load_first(k):
        part = pl.ds(k * (tokens // 2), tokens // 2)
        where = pl.ds(pl.multiple_of(mate_base, 128), half)
        return (
            pltpu.make_async_copy(a_hbm.at[0, 0, part, where], a_buf.at[0, 0, part], a_sem.at[2 * k]),
            pltpu.make_async_copy(
                g_hbm.at[0, 0, part, pl.ds(0, TILE)], g_buf.at[0, part, pl.ds(0, TILE)], g_sem.at[2 * k]
            ),
        )

    def remote(src, dst, sent, got, to):
        return pltpu.make_async_remote_copy(
            src_ref=src, dst_ref=dst, send_sem=sent, recv_sem=got,
            device_id={"dp": dev[to]}, device_id_type=MESH,
        )

    def place(u, w, row, count):
        return out.at[u // blocks, pl.ds(pl.multiple_of(row, sub), count), columns_of(u, w)]

    def hand(u, w):
        s, cols = u % 2, pl.ds(0, w)
        return remote(give.at[s, :, cols], take.at[s, :, cols], give_sem.at[s], take_sem.at[s], MATE)

    def ab(u, w, to):
        s, k, cols = u % SLOTS, u % 2, pl.ds(0, w)
        return remote(ab_out.at[k, to, :, cols], ab_in.at[s, to, :, cols], ab_sent.at[k], ab_got.at[s, to], to)

    def c(u, w, to):
        s, k, cols = u % SLOTS, u % 2, pl.ds(0, w)
        return remote(c_out.at[k, to, :, cols], c_in.at[s, to, :, cols], c_sent.at[k], c_got.at[s], to)

    def owned(u, w, to):
        s, ref = u % SLOTS, place(u, w, base + x * own, own)
        if to == MATE:
            return remote(ref, ref, mate_sent, mate_got, to)
        return remote(ref, ref, out_sent, own_got.at[s, to], to)

    def far(u, w, to):
        row = base + (xl * own if to == RIGHT else xr * own + sub)
        ref = place(u, w, row, sub)
        return remote(ref, ref, out_sent, far_got.at[u % SLOTS], to)

    def forward(u, w, k):
        ref = place(u, w, base + (xl, xr, opp)[k] * own, own)
        return remote(ref, ref, mate_sent, mate_got, MATE)

    def wait_for(ref, sem):
        pltpu.make_async_copy(ref, ref, sem).wait()

    def run(stage, u, also=True):
        here = (u >= 0) & (u < units) & also
        if wide == TILE:
            pl.when(here)(lambda: stage(u, TILE))
        else:
            pl.when(here & (u % blocks != fat))(lambda: stage(u, TILE))
            pl.when(here & (u % blocks == fat))(lambda: stage(u, wide))

    def run_late(stage, u):
        run(stage, u, u < units - 1)
        run(stage, units - 1, u == units - 2)

    def multiply(u, w, h, start=0, end=tokens):
        return lax.dot_general(
            a_buf[u // blocks % 2, h, start:end],
            g_buf[u % 2, start:end, :w],
            (((0,), (0,)), ((), ())),
            preferred_element_type=F32,
        )

    def stage_a(u, w):
        load_g(u, w).wait()
        give[u % 2, :, :w] = multiply(u, w, 0).astype(BF16)

    def stage_a2(u, w):
        hand(u, w).start()
        mine[:, :w] = multiply(u, w, 1)

    def stage_b(u, w):
        k = u % 2
        hand(u, w).wait()

        def total(owner, offset):
            where = pl.ds(pl.multiple_of(owner * own + offset, sub), sub)
            return mine[where, :w] + take[k, where, :w].astype(F32)

        ab_out[k, LEFT, :sub, :w] = total(opp, 0).astype(BF16)
        ab_out[k, LEFT, sub:, :w] = total(xl, sub).astype(BF16)
        ab(u, w, LEFT).start()
        ab_out[k, RIGHT, :sub, :w] = total(opp, sub).astype(BF16)
        ab_out[k, RIGHT, sub:, :w] = total(xr, 0).astype(BF16)
        ab(u, w, RIGHT).start()
        s = u % SLOTS
        keep[s, 0, :, :w] = total(xl, 0)
        keep[s, 1, :, :w] = total(xr, sub)
        keep[s, 2, :, :w] = total(x, 0)
        keep[s, 3, :, :w] = total(x, sub)

    def stage_b0(u, w):
        wait_for(ab_out.at[u % 2, :, :, pl.ds(0, w)], ab_sent.at[u % 2])

    def stage_c(u, w):
        s, k = u % SLOTS, u % 2
        for to in (LEFT, RIGHT):
            ab(u, w, to).wait_recv()
            c_out[k, to, :, :w] = (keep[s, to, :, :w] + ab_in[s, to, :sub, :w].astype(F32)).astype(BF16)
            c(u, w, to).start()
        for to in (LEFT, RIGHT):
            keep[s, 3 - to, :, :w] += ab_in[s, to, sub:, :w].astype(F32)

    def stage_c0(u, w):
        wait_for(c_out.at[u % 2, :, :, pl.ds(0, w)], c_sent.at[u % 2])

    def stage_d(u, w):
        s = u % SLOTS
        wait_for(c_in.at[s, :, :, pl.ds(0, w)], c_got.at[s])
        for k in (0, 1):
            total = keep[s, 2 + k, :, :w] + c_in[s, k, :, :w].astype(F32)
            row = pl.ds(pl.multiple_of(base + x * own + k * sub, sub), sub)
            out[u // blocks, row, columns_of(u, w)] = total.astype(BF16)
        for to in (LEFT, RIGHT, MATE):
            owned(u, w, to).start()

    def stage_e(u, w):
        owned(u, w, RIGHT).wait_recv()
        far(u, w, RIGHT).start()
        owned(u, w, LEFT).wait_recv()
        far(u, w, LEFT).start()
        forward(u, w, 0).start()
        forward(u, w, 1).start()

    def stage_g(u, w):
        wait_for(place(u, w, base + opp * own, own), far_got.at[u % SLOTS])
        forward(u, w, 2).start()

    barrier = pltpu.get_barrier_semaphore()
    for k in (0, 1):
        for copy in load_first(k):
            copy.start()
    load_a(0, 1).start()
    for to in (LEFT, RIGHT, MATE):
        pl.semaphore_signal(barrier, inc=1, device_id={"dp": dev[to]}, device_id_type=MESH)
    for copy in load_first(0):
        copy.wait()
    mine[:, :TILE] = multiply(0, TILE, 0, 0, tokens // 2)
    for copy in load_first(1):
        copy.wait()
    give[0, :, :TILE] = (mine[:, :TILE] + multiply(0, TILE, 0, tokens // 2)).astype(BF16)
    pl.semaphore_wait(barrier, 3)

    def iteration(t, carry):
        n, first = t // blocks, (t % blocks == 0) & (t < units)
        run(lambda u, w: load_g(u, w).start(), t + 1)

        @pl.when((t % blocks == 1) & (n + 1 < matrices))
        def _():
            for h in (0, 1):
                load_a(n + 1, h).start()

        pl.when(first & (t > 0))(lambda: load_a(n, 0).wait())
        run(stage_a, t, t > 0)
        pl.when(first)(lambda: load_a(n, 1).wait())
        run(stage_a2, t)
        run(stage_c0, t - 4, t - 4 != units - 3)
        run(stage_c0, units - 3, t == units)
        run_late(stage_c, t - 2)
        run(stage_b0, t - 2)
        run(stage_b, t)
        run_late(stage_d, t - 3)
        run_late(stage_e, t - 4)
        run_late(stage_g, t - 5)
        return carry

    lax.fori_loop(0, units + 4, iteration, 0)
    wait_for(out.at[:, pl.ds(pl.multiple_of(base, half), half), :], mate_sent)
    wait_for(out.at[:, pl.ds(0, 3 * own), :], out_sent)
    wait_for(out.at[:, pl.ds(pl.multiple_of(mate_base, half), half), :], mate_got)


def solution(mesh):
    chips = mesh.shape["dp"] // CORES

    def device(a, g):
        _, matrices, tokens, rows = a.shape
        columns = g.shape[-1]
        wide = cut(columns)[2]
        half = rows // CORES
        own = half // chips
        sub = own // 2
        dma = pltpu.SemaphoreType.DMA
        sums = pl.pallas_call(
            functools.partial(kernel, chips),
            out_shape=pltpu.VMEM((matrices, rows, columns), BF16),
            in_specs=[pl.BlockSpec(memory_space=pltpu.HBM)] * 2,
            out_specs=pl.BlockSpec(memory_space=pltpu.VMEM),
            scratch_shapes=[
                pltpu.VMEM((2, CORES, tokens, half), BF16),
                pltpu.VMEM((2, tokens, wide), BF16),
                pltpu.VMEM((half, wide), F32),
                pltpu.VMEM((2, half, wide), BF16),
                pltpu.VMEM((2, half, wide), BF16),
                pltpu.VMEM((SLOTS, 4, sub, wide), F32),
                pltpu.VMEM((2, 2, own, wide), BF16),
                pltpu.VMEM((SLOTS, 2, own, wide), BF16),
                pltpu.VMEM((2, 2, sub, wide), BF16),
                pltpu.VMEM((SLOTS, 2, sub, wide), BF16),
                dma((3,)), dma((3,)), dma((2,)), dma((2,)), dma((2,)), dma((SLOTS, 2)), dma((2,)), dma((SLOTS,)),
                dma((SLOTS, 2)), dma((SLOTS,)), dma, dma, dma,
            ],
            compiler_params=pltpu.CompilerParams(
                collective_id=0, has_side_effects=True, vmem_limit_bytes=37 * 2**20
            ),
            cost_estimate=pl.CostEstimate(
                flops=2 * matrices * tokens * rows * columns,
                bytes_accessed=2 * matrices * tokens * (rows + columns),
                transcendentals=0,
            ),
        )(a, g)

        def store(held, result, sem):
            parts = [(n, pl.ds(k * half // 2, half // 2)) for n in range(matrices) for k in range(2 * rows // half)]
            for p in parts:
                pltpu.make_async_copy(held.at[p], result.at[p], sem).start()
            pltpu.make_async_copy(held, result, sem).wait()

        return pl.pallas_call(
            store,
            out_shape=jax.ShapeDtypeStruct(sums.shape, BF16),
            in_specs=[pl.BlockSpec(memory_space=pltpu.VMEM)],
            out_specs=pl.BlockSpec(memory_space=pltpu.HBM),
            scratch_shapes=[dma],
            compiler_params=pltpu.CompilerParams(vmem_limit_bytes=2**20),
        )(pltpu.with_memory_space_constraint(sums, pltpu.VMEM))

    return jax.shard_map(
        device, mesh=mesh, in_specs=(P(("rep", "dp")), P(("rep", "dp"))), out_specs=P("rep"), check_vma=False
    )
```
